32 devices in a mesh: dp: 16 (over z, x, core), gene: 2 (over y).
Axes of the slice: x: 2, y: 2, z: 4, core: 2. Of those that a mesh axis runs over, the one named last changes fastest.
Arguments:
- counts: int32 [4096, 13500], P('dp', 'gene'), may hold values from 0 to 15, as said below
- coords: float32 [4096, 2], P(('dp', 'gene')), may hold values from 0 to 100
- segments: int32 [32, 128], P(('dp', 'gene')), may hold values from 0 to 3, never falling along the last dimension, each value on 1 to 64 neighbouring positions
- noise: float32 [4096, 512], P(('dp', 'gene')), may hold values from -6 to 6
- embed_table: bfloat16 [13500, 1024], P('gene'), may hold values from -0.0546875 to 0.0546875
- ln1_gain: float32 [1024], replicated, may hold values from 0.5 to 1.5
- ln1_bias: float32 [1024], replicated, may hold values from -1 to 1
- w_qkv: bfloat16 [1024, 3072], replicated, may hold values from -0.1875 to 0.1875
- w_out: bfloat16 [1024, 1024], replicated, may hold values from -0.375 to 0.375
- ln2_gain: float32 [1024], replicated, may hold values from 0.5 to 1.5
- ln2_bias: float32 [1024], replicated, may hold values from -1 to 1
- w_up: bfloat16 [1024, 4096], replicated, may hold values from -0.1875 to 0.1875
- w_down: bfloat16 [4096, 1024], replicated, may hold values from -0.09375 to 0.09375
- w_latent: bfloat16 [1024, 1024], replicated, may hold values from -0.09375 to 0.09375
- mix_means: float32 [16, 512], replicated, may hold values from -0.4 to 0.4
- mix_logits: float32 [16], replicated, may hold values from -4 to 4
- w_decode: bfloat16 [512, 13500], P(None, 'gene'), may hold values from -0.25 to 0.25
Outputs:
- block_out: bfloat16 [4096, 1024], P(('dp', 'gene'))
- loss: float32 [], replicated
- grad_input: float32 [4096, 1024], P(('dp', 'gene'))
- grad_table: float32 [1024, 13500], P('dp', 'gene')
- grad_decode: float32 [512, 13500], P('dp', 'gene')
- grad_qkv: float32 [1024, 3072], P('dp', 'gene')
- grad_out: float32 [1024, 1024], P('dp', 'gene')
- grad_ln1_gain: float32 [1024], replicated
- grad_ln1_bias: float32 [1024], replicated
- grad_ln2_gain: float32 [1024], replicated
- grad_ln2_bias: float32 [1024], replicated
- grad_up: float32 [1024, 4096], P('dp', 'gene')
- grad_down: float32 [4096, 1024], P('dp', 'gene')
- grad_latent: float32 [1024, 1024], P('dp', 'gene')
- grad_means: float32 [16, 512], replicated
- grad_logits: float32 [16], replicated
The draws below stay inside these ranges and needn't reach their ends.
Inputs may be any that keep to these rules, and one draw needn't show every extreme that they name: `counts`: about a quarter of the entries are nonzero. `segments`: along each row the ids never fall; each of the 4 slides of a row holds 1 to 64 cells, one exactly 64.
All inputs are finite; a program needn't handle non-finite values.
Results may differ from the reference program's by a relative error of at most 0.013.
Values may be sent and summed in bfloat16 or wider, within the bound.
A program may use at most 384 MiB of HBM per device.

```python
import math
import jax
import jax.numpy as jnp
import numpy as np
from jax import lax

D = 1024
FF = 4096
HEADS = 16
HDIM = 64
LAT = 512
NCOMP = 16
G = 13500
TOK_DEV = 128
SLIDES = 4
SEQS = 32
CELLS = 4096


def draw_counts(key, part):
    first, second = jax.random.split(jax.random.fold_in(key, 7))
    level = jax.random.randint(first, (CELLS, G), 1, 16)
    keep = jax.random.randint(second, (CELLS, G), 0, 4)
    return jnp.where(keep == 0, level, 0).astype(jnp.int32)


def block_scale(own_key, dims, cuts, low, largest):
    def one(axis_at, parts):
        steps = jax.random.uniform(jax.random.fold_in(jax.random.fold_in(own_key, 6), axis_at), (parts,), jnp.float32, low / len(cuts), largest / len(cuts))
        return jnp.repeat(jnp.exp(steps), dims[axis_at] // parts).reshape((-1,) + (1,) * (len(dims) - axis_at - 1))

    factor_of = one(*cuts[0])
    for cut in cuts[1:]:
        factor_of = factor_of * one(*cut)
    return factor_of


def split_up(count, total, most, skew):
    loads = [(1 << 20) // math.isqrt(standing ** skew) + 1 for standing in range(2, count + 1)]
    rest, given = total - most - (count - 1), [1] * (count - 1)
    while rest > 0:
        movable = [i for i in range(count - 1) if given[i] < most]
        whole, budget = sum([loads[i] for i in movable]), rest
        for i in movable:
            more = min(most - given[i], max(1, budget * loads[i] // whole), rest)
            given[i] = given[i] + more
            rest = rest - more
    return np.array([most] + given)


def ragged_sizes(rng, count, total, limit, lean):
    if count == 2:
        one = jax.random.randint(rng, (), max(1, total - limit), min(limit, total - 1) + 1)
        return jnp.stack([one, total - one])
    tallies = jnp.asarray(split_up(count, total, limit, lean), jnp.int32)
    twos = (count - 1) // 2
    donor, sink = tallies[1:1 + 2 * twos:2], tallies[2:2 + 2 * twos:2]
    margin = jnp.minimum(donor - 1, limit - sink)
    passed = jax.random.randint(jax.random.fold_in(rng, 1), (twos,), 0, 1 << 20) % (margin + 1)
    tallies = tallies.at[1:1 + 2 * twos:2].set(donor - passed).at[2:2 + 2 * twos:2].set(sink + passed)
    return tallies[jax.random.permutation(jax.random.fold_in(rng, 2), count)]


def gaussian(rng, shape, width, reach, cuts=(), kind=jnp.bfloat16):
    loudness = block_scale(rng, shape, cuts, -0.22, 0.18) if cuts else 1.0
    drawn = jax.random.normal(rng, shape, jnp.float32) * width * loudness
    return jnp.minimum(jnp.maximum(drawn, -reach), reach).astype(kind)


def setup_inputs(seed: int = 0) -> dict:
    key_of = jax.random.split(jax.random.key(seed), 18)
    counts = draw_counts(jax.random.fold_in(key_of[17], 71), 0)
    coords = jnp.clip(100.0 * jax.random.uniform(key_of[1], (CELLS, 2), jnp.float32) ** block_scale(key_of[1], (CELLS, 2), ((0, 32),), -0.2, 0.2), 0.0, 100.0)
    segments = jax.vmap(lambda own: jnp.searchsorted(jnp.cumsum(ragged_sizes(own, SLIDES, TOK_DEV, TOK_DEV // 2, 2)), jnp.arange(TOK_DEV), side="right"))(jax.random.split(key_of[2], SEQS)).reshape((SEQS, TOK_DEV)).astype(jnp.int32)
    noise = gaussian(key_of[3], (CELLS, LAT), 1.0, 6.0, ((0, 32),), jnp.float32)
    embed_table = gaussian(key_of[4], (G, D), G ** -0.5, 0.0546875, ((0, 2),))
    ln1_gain = jnp.clip(1.0 + 0.1 * jax.random.normal(key_of[5], (D,), jnp.float32), 0.5, 1.5)
    ln1_bias = gaussian(key_of[6], (D,), 0.2, 1.0, (), jnp.float32)
    w_qkv = gaussian(key_of[7], (D, 3 * D), D ** -0.5, 0.1875)
    w_out = gaussian(key_of[8], (D, D), (D // 4) ** -0.5, 0.375)
    ln2_gain = jnp.clip(1.0 + 0.1 * jax.random.normal(key_of[9], (D,), jnp.float32), 0.5, 1.5)
    ln2_bias = gaussian(key_of[10], (D,), 0.2, 1.0, (), jnp.float32)
    w_up = gaussian(key_of[11], (D, FF), D ** -0.5, 0.1875)
    w_down = gaussian(key_of[12], (FF, D), FF ** -0.5, 0.09375)
    w_latent = gaussian(key_of[13], (D, 2 * LAT), (4 * D) ** -0.5, 0.09375)
    mix_means = gaussian(key_of[14], (NCOMP, LAT), 0.07, 0.4, (), jnp.float32)
    mix_logits = gaussian(key_of[15], (NCOMP,), 1.0, 4.0, (), jnp.float32)
    w_decode = gaussian(key_of[16], (LAT, G), LAT ** -0.5, 0.25, ((1, 2),))
    return dict(counts=counts, coords=coords, segments=segments, noise=noise, embed_table=embed_table, ln1_gain=ln1_gain, ln1_bias=ln1_bias, w_qkv=w_qkv, w_out=w_out, ln2_gain=ln2_gain, ln2_bias=ln2_bias, w_up=w_up, w_down=w_down, w_latent=w_latent, mix_means=mix_means, mix_logits=mix_logits, w_decode=w_decode)


@jax.custom_vjp
def low(v):
    return lax.optimization_barrier(v.astype(jnp.bfloat16)).astype(jnp.float32)

@jax.custom_vjp
def low_back(v):
    return v

def low_keep(v):
    return (low(v), None)

def low_pass(kept, grad):
    return (grad,)

def back_keep(v):
    return (v, None)

def back_low(kept, grad):
    return (low(grad),)
low.defvjp(low_keep, low_pass)
low_back.defvjp(back_keep, back_low)

def product(left, right):
    return jnp.dot(left, right, precision=lax.Precision.HIGHEST, preferred_element_type=jnp.float32)

def position_code(coords):
    quarter = D // 4
    freq = jnp.exp(-jnp.arange(quarter, dtype=jnp.float32) * (math.log(100.0) / quarter))
    along_x = coords[:, 0:1] * freq[None, :]
    along_y = coords[:, 1:2] * freq[None, :]
    return jnp.concatenate([jnp.sin(along_x), jnp.cos(along_x), jnp.sin(along_y), jnp.cos(along_y)], axis=1)

def layer_norm(values, gain, bias):
    center = values - lax.optimization_barrier(jnp.mean(values, axis=-1, keepdims=True))
    spread = lax.rsqrt(lax.optimization_barrier(jnp.mean(center * center, axis=-1, keepdims=True)) + 1e-05)
    return center * spread * gain + bias

def reference(counts, coords, segments, noise, embed_table, ln1_gain, ln1_bias, w_qkv, w_out, ln2_gain, ln2_bias, w_up, w_down, w_latent, mix_means, mix_logits, w_decode):
    params = tuple((item.astype(jnp.float32) for item in (embed_table, ln1_gain, ln1_bias, w_qkv, w_out, ln2_gain, ln2_bias, w_up, w_down, w_latent, mix_means, mix_logits, w_decode)))
    per = math.gcd(SEQS, 8)
    rows = per * TOK_DEV
    groups = SEQS // per
    factor = 1.0 / (CELLS * G)
    scale = HDIM ** (-0.5)

    def forward(params, delta):
        table, gain1, bias1, wqkv, wout, gain2, bias2, wup, wdown, wlat, means, logits, wdec = params
        log_weight = jax.nn.log_softmax(logits)

        def one_group(total, index):
            start = index * rows
            counts_rows = lax.dynamic_slice_in_dim(counts, start, rows, 0)
            coord_rows = lax.dynamic_slice_in_dim(coords, start, rows, 0)
            noise_rows = lax.dynamic_slice_in_dim(noise, start, rows, 0)
            delta_rows = lax.dynamic_slice_in_dim(delta, start, rows, 0)
            seg_rows = lax.dynamic_slice_in_dim(segments, index * per, per, 0)
            target = jnp.log1p(counts_rows.astype(jnp.float32))
            expr_low = low(target)
            embedded = low_back(product(expr_low, table))
            state_in = embedded + position_code(coord_rows) + delta_rows
            normed1 = low(layer_norm(state_in, gain1, bias1))
            qkv = low_back(low(product(normed1, wqkv)))
            qkv = qkv.reshape(per, TOK_DEV, 3, HEADS, HDIM)
            query, keys, values = (qkv[:, :, 0], qkv[:, :, 1], qkv[:, :, 2])
            raw = jnp.einsum('sqhd,skhd->shqk', query, keys, precision=lax.Precision.HIGHEST) * scale
            same = (seg_rows[:, :, None] == seg_rows[:, None, :])[:, None]
            scores = low_back(jnp.where(same, raw, -1e+30))
            probs = low(jax.nn.softmax(scores, axis=-1))
            attended = jnp.einsum('shqk,skhd->sqhd', probs, values, precision=lax.Precision.HIGHEST).reshape(rows, D)
            attended = low_back(low(attended))
            state_mid = state_in + low_back(product(attended, wout))
            normed2 = low(layer_norm(state_mid, gain2, bias2))
            pre_act = low_back(product(normed2, wup))
            active = low(jax.nn.gelu(pre_act, approximate=False))
            state_out = state_mid + low_back(product(active, wdown))
            latent = low_back(product(low(state_out), wlat))
            center = latent[:, :LAT]
            log_var = latent[:, LAT:]
            sample = center + jnp.exp(0.5 * log_var) * noise_rows
            predicted = low_back(product(low(sample), wdec))
            error = predicted - target
            recon = 0.5 * jnp.sum(error * error)
            dist = lax.optimization_barrier(jnp.sum(sample * sample, axis=1, keepdims=True)) - 2.0 * product(sample, means.T) + lax.optimization_barrier(jnp.sum(means * means, axis=1))[None, :]
            mix_score = log_weight[None, :] - 0.5 * dist
            mixture = jnp.sum(-0.5 * log_var) - jnp.sum(jax.scipy.special.logsumexp(mix_score, axis=1))
            return (total + factor * (recon + mixture), state_out)
        total, outs = lax.scan(jax.checkpoint(one_group), jnp.zeros((), jnp.float32), jnp.arange(groups, dtype=jnp.int32))
        return (total, outs.reshape(CELLS, D))
    delta = jnp.zeros((CELLS, D), jnp.float32)
    (loss, state_out), pullback = jax.vjp(forward, params, delta)
    grads, grad_input = pullback((jnp.ones((), jnp.float32), jnp.zeros_like(state_out)))
    g_table, g_gain1, g_bias1, g_qkv, g_out, g_gain2, g_bias2, g_up, g_down, g_lat, g_means, g_logits, g_dec = grads
    return (state_out.astype(jnp.bfloat16), loss, grad_input, g_table.T, g_dec, g_qkv, g_out, g_gain1, g_bias1, g_gain2, g_bias2, g_up, g_down, g_lat, g_means, g_logits)
```

```python
import math

import jax
import jax.numpy as jnp
from jax import lax
from jax.sharding import PartitionSpec as P

D = 1024
HEADS = 16
HDIM = 64
LAT = 512
G = 13500


ln_eps = 1e-05
root_half = 0.7071067811865476
inv_root_two_pi = 0.3989422804014327
mask_floor = -1e30


def product(left, right):
    return jnp.dot(left, right, preferred_element_type=jnp.float32)


def product_left(left, right):
    return lax.dot_general(
        left, right, (((0,), (0,)), ((), ())), preferred_element_type=jnp.float32
    )


def product_right(left, right):
    return lax.dot_general(
        left, right, (((1,), (1,)), ((), ())), preferred_element_type=jnp.float32
    )


def precise(left, right):
    return jnp.dot(left, right, precision=lax.Precision.HIGHEST, preferred_element_type=jnp.float32)


def position_code(coords):
    quarter = D // 4
    freq = jnp.exp(-jnp.arange(quarter, dtype=jnp.float32) * (math.log(100.0) / quarter))
    along_x = coords[:, 0:1] * freq[None, :]
    along_y = coords[:, 1:2] * freq[None, :]
    return jnp.concatenate(
        [jnp.sin(along_x), jnp.cos(along_x), jnp.sin(along_y), jnp.cos(along_y)], axis=1
    )


def norm_forward(values, gain, bias):
    center = values - jnp.mean(values, axis=-1, keepdims=True)
    spread = lax.rsqrt(jnp.mean(center * center, axis=-1, keepdims=True) + ln_eps)
    normal = center * spread
    return (normal * gain + bias, normal, spread)


def norm_backward(grad_out, normal, spread, gain):
    grad_normal = grad_out * gain
    inner = (
        grad_normal
        - jnp.mean(grad_normal, axis=-1, keepdims=True)
        - normal * jnp.mean(grad_normal * normal, axis=-1, keepdims=True)
    )
    return (spread * inner, jnp.sum(grad_out * normal, axis=0), jnp.sum(grad_out, axis=0))


def shards(
    counts,
    coords,
    segments,
    noise,
    embed_table,
    ln1_gain,
    ln1_bias,
    w_qkv,
    w_out,
    ln2_gain,
    ln2_bias,
    w_up,
    w_down,
    w_latent,
    mix_means,
    mix_logits,
    w_decode,
):
    cells = coords.shape[0]
    all_cells = cells * lax.axis_size("dp") * lax.axis_size("gene")
    factor = 1.0 / (all_cells * G)
    scale = HDIM ** (-0.5)
    target = jnp.log1p(counts.astype(jnp.float32))
    expr_low = target.astype(jnp.bfloat16)
    embedded = lax.psum_scatter(
        product(expr_low, embed_table), "gene", scatter_dimension=0, tiled=True
    )
    state_in = embedded + position_code(coords)
    normed1, unit1, spread1 = norm_forward(state_in, ln1_gain, ln1_bias)
    normed1 = normed1.astype(jnp.bfloat16)
    qkv_low = product(normed1, w_qkv).astype(jnp.bfloat16)
    query = qkv_low[:, :D].reshape(cells, HEADS, HDIM)
    keys = qkv_low[:, D : 2 * D].reshape(cells, HEADS, HDIM)
    values = qkv_low[:, 2 * D :].reshape(cells, HEADS, HDIM)
    slide = segments[0]
    same = (slide[:, None] == slide[None, :])[None]
    scores = jnp.einsum("qhd,khd->hqk", query, keys, preferred_element_type=jnp.float32) * scale
    scores = jnp.where(same, scores, mask_floor)
    peak = jnp.max(scores, axis=-1, keepdims=True)
    expo = jnp.exp(scores - peak)
    probs = expo / jnp.sum(expo, axis=-1, keepdims=True)
    probs_low = probs.astype(jnp.bfloat16)
    attended = jnp.einsum("hqk,khd->qhd", probs_low, values, preferred_element_type=jnp.float32)
    attended = attended.reshape(cells, D).astype(jnp.bfloat16)
    state_mid = state_in + product(attended, w_out)
    normed2, unit2, spread2 = norm_forward(state_mid, ln2_gain, ln2_bias)
    normed2 = normed2.astype(jnp.bfloat16)
    pre_act = product(normed2, w_up)
    cumul = 0.5 * (1.0 + lax.erf(pre_act * root_half))
    active = (pre_act * cumul).astype(jnp.bfloat16)
    state_out = state_mid + product(active, w_down)
    out_low = state_out.astype(jnp.bfloat16)
    latent = product(out_low, w_latent)
    center = latent[:, :LAT]
    log_var = latent[:, LAT:]
    deviation = jnp.exp(0.5 * log_var)
    sample = center + deviation * noise
    sample_low = sample.astype(jnp.bfloat16)
    sample_all = lax.all_gather(sample_low, "gene", axis=0, tiled=True)
    predicted = product(sample_all, w_decode)
    error = predicted - target
    recon = 0.5 * jnp.sum(error * error)
    grad_pred = (factor * error).astype(jnp.bfloat16)
    grad_dec_local = product_left(sample_all, grad_pred)
    grad_sample = lax.psum_scatter(
        product_right(grad_pred, w_decode), "gene", scatter_dimension=0, tiled=True
    )
    log_weight = jax.nn.log_softmax(mix_logits)
    dist = (
        jnp.sum(sample * sample, axis=1, keepdims=True)
        - 2.0 * precise(sample, mix_means.T)
        + jnp.sum(mix_means * mix_means, axis=1)[None, :]
    )
    mix_score = log_weight[None, :] - 0.5 * dist
    top = jnp.max(mix_score, axis=1, keepdims=True)
    shifted = jnp.exp(mix_score - top)
    totals = jnp.sum(shifted, axis=1, keepdims=True)
    share = shifted / totals
    mixture = jnp.sum(-0.5 * log_var) - jnp.sum(top + jnp.log(totals))
    loss_part = factor * (recon + mixture)
    grad_sample = grad_sample + factor * (sample - precise(share, mix_means))
    share_sum = jnp.sum(share, axis=0)
    grad_means_local = factor * (share_sum[:, None] * mix_means - precise(share.T, sample))
    weight_sum = -factor * share_sum
    grad_logits_local = weight_sum - jnp.exp(log_weight) * jnp.sum(weight_sum)
    grad_logvar = -0.5 * factor + grad_sample * 0.5 * deviation * noise
    grad_lat_low = jnp.concatenate([grad_sample, grad_logvar], axis=1).astype(jnp.bfloat16)
    grad_w_latent = product_left(out_low, grad_lat_low)
    grad_state = product_right(grad_lat_low, w_latent)
    grad_branch = grad_state.astype(jnp.bfloat16)
    grad_w_down = product_left(active, grad_branch)
    grad_active = product_right(grad_branch, w_down)
    slope = cumul + pre_act * jnp.exp(-0.5 * pre_act * pre_act) * inv_root_two_pi
    grad_pre = (grad_active * slope).astype(jnp.bfloat16)
    grad_w_up = product_left(normed2, grad_pre)
    grad_normed2 = product_right(grad_pre, w_up)
    back_two, grad_gain2, grad_bias2 = norm_backward(grad_normed2, unit2, spread2, ln2_gain)
    grad_state = grad_state + back_two
    grad_attn_low = grad_state.astype(jnp.bfloat16)
    grad_w_out = product_left(attended, grad_attn_low)
    grad_attended = (
        product_right(grad_attn_low, w_out).astype(jnp.bfloat16).reshape(cells, HEADS, HDIM)
    )
    grad_probs = jnp.einsum(
        "qhd,khd->hqk", grad_attended, values, preferred_element_type=jnp.float32
    )
    row_inner = jnp.sum(probs * grad_probs, axis=-1, keepdims=True)
    grad_scores = (probs * (grad_probs - row_inner)).astype(jnp.bfloat16)
    grad_query = (
        jnp.einsum("hqk,khd->qhd", grad_scores, keys, preferred_element_type=jnp.float32) * scale
    )
    grad_keys = (
        jnp.einsum("hqk,qhd->khd", grad_scores, query, preferred_element_type=jnp.float32) * scale
    )
    grad_values = jnp.einsum(
        "hqk,qhd->khd", probs_low, grad_attended, preferred_element_type=jnp.float32
    )
    grad_qkv_low = jnp.concatenate(
        [grad_query.reshape(cells, D), grad_keys.reshape(cells, D), grad_values.reshape(cells, D)],
        axis=1,
    ).astype(jnp.bfloat16)
    grad_w_qkv = product_left(normed1, grad_qkv_low)
    grad_normed1 = product_right(grad_qkv_low, w_qkv)
    back_one, grad_gain1, grad_bias1 = norm_backward(grad_normed1, unit1, spread1, ln1_gain)
    grad_input = grad_state + back_one
    grad_embed_low = grad_input.astype(jnp.bfloat16)
    grad_table_local = product_left(
        lax.all_gather(grad_embed_low, "gene", axis=0, tiled=True), expr_low
    )
    table_part, decode_part = (
        lax.psum_scatter(
            grad_table_local.astype(jnp.bfloat16), "dp", scatter_dimension=0, tiled=True
        ).astype(jnp.float32),
        lax.psum_scatter(
            grad_dec_local.astype(jnp.bfloat16), "dp", scatter_dimension=0, tiled=True
        ).astype(jnp.float32),
    )
    gene_qkv, gene_out, gene_up, gene_down, gene_latent = (
        lax.psum_scatter(
            grad_w_qkv.astype(jnp.bfloat16), "gene", scatter_dimension=1, tiled=True
        ),
        lax.psum_scatter(
            grad_w_out.astype(jnp.bfloat16), "gene", scatter_dimension=1, tiled=True
        ),
        lax.psum_scatter(
            grad_w_up.astype(jnp.bfloat16), "gene", scatter_dimension=1, tiled=True
        ),
        lax.psum_scatter(
            grad_w_down.astype(jnp.bfloat16), "gene", scatter_dimension=1, tiled=True
        ),
        lax.psum_scatter(
            grad_w_latent.astype(jnp.bfloat16), "gene", scatter_dimension=1, tiled=True
        ),
    )
    sum_qkv, sum_out, sum_up, sum_down, sum_latent = (
        lax.psum_scatter(gene_qkv, "dp", scatter_dimension=0, tiled=True).astype(
            jnp.float32
        ),
        lax.psum_scatter(gene_out, "dp", scatter_dimension=0, tiled=True).astype(
            jnp.float32
        ),
        lax.psum_scatter(gene_up, "dp", scatter_dimension=0, tiled=True).astype(
            jnp.float32
        ),
        lax.psum_scatter(gene_down, "dp", scatter_dimension=0, tiled=True).astype(
            jnp.float32
        ),
        lax.psum_scatter(gene_latent, "dp", scatter_dimension=0, tiled=True).astype(
            jnp.float32
        ),
    )
    loss_total, logits_total, means_total, sum_gain1, sum_bias1, sum_gain2, sum_bias2 = lax.psum(
        (
            loss_part,
            grad_logits_local,
            grad_means_local,
            grad_gain1,
            grad_bias1,
            grad_gain2,
            grad_bias2,
        ),
        ("dp", "gene"),
    )
    return (
        state_out.astype(jnp.bfloat16),
        loss_total,
        grad_input,
        table_part,
        decode_part,
        sum_qkv,
        sum_out,
        sum_gain1,
        sum_bias1,
        sum_gain2,
        sum_bias2,
        sum_up,
        sum_down,
        sum_latent,
        means_total,
        logits_total,
    )


def solution(mesh):
    in_specs = (
        P("dp", "gene"),
        P(("dp", "gene"), None),
        P(("dp", "gene"), None),
        P(("dp", "gene"), None),
        P("gene", None),
        P(),
        P(),
        P(),
        P(),
        P(),
        P(),
        P(),
        P(),
        P(),
        P(),
        P(),
        P(None, "gene"),
    )
    out_specs = (
        P(("dp", "gene"), None),
        P(),
        P(("dp", "gene"), None),
        P("dp", "gene"),
        P("dp", "gene"),
        P("dp", "gene"),
        P("dp", "gene"),
        P(),
        P(),
        P(),
        P(),
        P("dp", "gene"),
        P("dp", "gene"),
        P("dp", "gene"),
        P(),
        P(),
    )
    return jax.shard_map(shards, mesh=mesh, in_specs=in_specs, out_specs=out_specs, check_vma=False)
```

```python
import functools
import math

import jax
import jax.numpy as jnp
from jax import lax
from jax.experimental import pallas as pl
from jax.experimental.pallas import tpu as pltpu
from jax.sharding import PartitionSpec as P


D = 1024
HEADS = 16
HDIM = 64
LAT = 512
G = 13500


ln_eps = 1e-05
root_half = 0.7071067811865476
inv_root_two_pi = 0.3989422804014327
mask_floor = -1e30


def product(left, right):
    return jnp.dot(left, right, preferred_element_type=jnp.float32)


def precise(left, right):
    return jnp.dot(left, right, precision=lax.Precision.HIGHEST, preferred_element_type=jnp.float32)


def position_code(coords):
    quarter = D // 4
    freq = jnp.exp(-jnp.arange(quarter, dtype=jnp.float32) * (math.log(100.0) / quarter))
    along_x = coords[:, 0:1] * freq[None, :]
    along_y = coords[:, 1:2] * freq[None, :]
    return jnp.concatenate(
        [jnp.sin(along_x), jnp.cos(along_x), jnp.sin(along_y), jnp.cos(along_y)], axis=1
    )


def norm_forward(values, gain, bias):
    center = values - jnp.mean(values, axis=-1, keepdims=True)
    spread = lax.rsqrt(jnp.mean(center * center, axis=-1, keepdims=True) + ln_eps)
    normal = center * spread
    return (normal * gain + bias, normal, spread)


def norm_backward(grad_out, normal, spread, gain):
    grad_normal = grad_out * gain
    inner = (
        grad_normal
        - jnp.mean(grad_normal, axis=-1, keepdims=True)
        - normal * jnp.mean(grad_normal * normal, axis=-1, keepdims=True)
    )
    return (spread * inner, jnp.sum(grad_out * normal, axis=0), jnp.sum(grad_out, axis=0))


def swap(values, axis, stride):
    size = lax.axis_size(axis)
    return lax.ppermute(values, axis, [(i, i ^ stride) for i in range(size)])


def contract(left, right, dims):
    return lax.dot_general(
        left, right, ((dims[0], dims[1]), ((), ())), preferred_element_type=jnp.float32
    )


def half(values, bit, axis):
    size = values.shape[axis] // 2
    low = lax.slice_in_dim(values, 0, size, axis=axis)
    high = lax.slice_in_dim(values, size, 2 * size, axis=axis)
    return jnp.where(bit == 0, low, high)


def column_blocks(values, bit, parts):
    width = values.shape[1] // (2 * parts)
    chosen = []
    for i in range(parts):
        low = values[:, 2 * i * width : (2 * i + 1) * width]
        high = values[:, (2 * i + 1) * width : (2 * i + 2) * width]
        chosen.append(jnp.where(bit == 0, low, high))
    return jnp.concatenate(chosen, axis=1)


def weight_kernel(pieces, blocks, width, turn, bits, *refs):
    lefts, rights = refs[:pieces], refs[pieces : 2 * pieces]
    send, keep, turned = refs[2 * pieces :]

    @pl.when(pl.program_id(0) == 0)
    def _():
        turned[...] = jnp.concatenate([ref[...] for ref in lefts], axis=0).T

    right = jnp.concatenate([ref[...] for ref in rights], axis=1 if turn else 0)
    total = lax.dot_general(
        turned[...],
        right,
        (((1,), (1 if turn else 0,)), ((), ())),
        preferred_element_type=jnp.float32,
    )
    first = bits[0] == 0
    for i in range(blocks):
        low = total[2 * i * width : (2 * i + 1) * width]
        high = total[(2 * i + 1) * width : (2 * i + 2) * width]
        keep[i] = jnp.where(first, low, high).astype(jnp.bfloat16)
        send[i] = jnp.where(first, high, low).astype(jnp.bfloat16)


def in_place(values):
    return pltpu.with_memory_space_constraint(values, pltpu.HBM)


def inside(tile, genes):
    row = lax.broadcasted_iota(jnp.int32, (tile, 1), 0) + pl.program_id(0) * tile
    return row < genes


def embed_kernel(genes, counts, table, expr, total):
    tile = counts.shape[0]
    valid = inside(tile, genes)
    logs = jnp.where(valid, jnp.log(1.0 + counts[...].astype(jnp.float32)), 0.0)
    low = logs.astype(jnp.bfloat16)
    expr[...] = low
    rows = jnp.where(valid, table[...], jnp.zeros_like(table[...]))
    part = jnp.dot(low.T, rows, preferred_element_type=jnp.float32)

    @pl.when(pl.program_id(0) == 0)
    def _():
        total[...] = part

    @pl.when(pl.program_id(0) > 0)
    def _():
        total[...] += part


def embed_cells(counts, table, tile):
    genes, cells = counts.shape
    width = table.shape[1]
    return pl.pallas_call(
        functools.partial(embed_kernel, genes),
        out_shape=(
            jax.ShapeDtypeStruct((genes, cells), jnp.bfloat16),
            jax.ShapeDtypeStruct((cells, width), jnp.float32),
        ),
        grid=(pl.cdiv(genes, tile),),
        in_specs=[
            pl.BlockSpec((tile, cells), lambda j: (j, 0)),
            pl.BlockSpec((tile, width), lambda j: (j, 0)),
        ],
        out_specs=[
            pl.BlockSpec((tile, cells), lambda j: (j, 0)),
            pl.BlockSpec((cells, width), lambda j: (0, 0)),
        ],
        compiler_params=pltpu.CompilerParams(vmem_limit_bytes=24 * 1024 * 1024),
        cost_estimate=pl.CostEstimate(
            flops=2 * genes * cells * width,
            bytes_accessed=genes * (6 * cells + 2 * width),
            transcendentals=genes * cells,
        ),
        name="e",
    )(in_place(counts), in_place(table))


def decode_kernel(genes, factor, blocks, width, bits, counts, table, sample, *refs):
    send, keep, grad, square, turned = refs
    tile = counts.shape[0]
    start = pl.program_id(0) == 0

    @pl.when(start)
    def _():
        turned[...] = sample[...].T
        grad[...] = jnp.zeros_like(grad)
        square[...] = jnp.zeros_like(square)

    valid = inside(tile, genes)
    rows = jnp.where(valid, table[...], jnp.zeros_like(table[...]))
    predicted = jnp.dot(rows, turned[...], preferred_element_type=jnp.float32)
    logs = jnp.log(1.0 + counts[...].astype(jnp.float32))
    error = jnp.where(valid, predicted - logs, 0.0)
    square[...] += jnp.sum(error * error, axis=0, keepdims=True)
    low = (factor * error).astype(jnp.bfloat16).T
    grad[...] += jnp.dot(low, rows, preferred_element_type=jnp.float32)
    total = jnp.dot(turned[...], low, preferred_element_type=jnp.float32)
    first = bits[0] == 0
    for i in range(blocks):
        even = total[2 * i * width : (2 * i + 1) * width]
        odd = total[(2 * i + 1) * width : (2 * i + 2) * width]
        keep[i] = jnp.where(first, even, odd).astype(jnp.bfloat16)
        send[i] = jnp.where(first, odd, even).astype(jnp.bfloat16)


def decode_genes(counts, table, sample, bits, factor, blocks, tile):
    genes, cells = counts.shape
    latents = sample.shape[1]
    width = latents // (2 * blocks)
    halves = jax.ShapeDtypeStruct((blocks, width, genes), jnp.bfloat16)
    half_spec = pl.BlockSpec((blocks, width, tile), lambda j, bits: (0, 0, j))
    whole = lambda j, bits: (0, 0)
    rows = lambda j, bits: (j, 0)
    return pl.pallas_call(
        functools.partial(decode_kernel, genes, factor, blocks, width),
        out_shape=(
            halves,
            halves,
            jax.ShapeDtypeStruct((cells, latents), jnp.float32),
            jax.ShapeDtypeStruct((1, cells), jnp.float32),
        ),
        grid_spec=pltpu.PrefetchScalarGridSpec(
            num_scalar_prefetch=1,
            grid=(pl.cdiv(genes, tile),),
            in_specs=[
                pl.BlockSpec((tile, cells), rows),
                pl.BlockSpec((tile, latents), rows),
                pl.BlockSpec((cells, latents), whole),
            ],
            out_specs=[
                half_spec,
                half_spec,
                pl.BlockSpec((cells, latents), whole),
                pl.BlockSpec((1, cells), whole),
            ],
            scratch_shapes=[pltpu.VMEM((latents, cells), jnp.bfloat16)],
        ),
        compiler_params=pltpu.CompilerParams(vmem_limit_bytes=24 * 1024 * 1024),
        cost_estimate=pl.CostEstimate(
            flops=6 * genes * cells * latents,
            bytes_accessed=genes * (4 * cells + 4 * latents),
            transcendentals=genes * cells,
        ),
        name="d",
    )(bits, in_place(counts), in_place(table), sample)


def weight_grad(lefts, rights, bits, blocks, tile, columns, turn=False):
    pieces = len(lefts)
    rows = lefts[0][1][-1]
    depth = sum(left[1][-2] for left in lefts)
    width = rows // (2 * blocks)
    out = jax.ShapeDtypeStruct((blocks, width, columns), jnp.bfloat16)
    out_spec = pl.BlockSpec((blocks, width, tile), lambda j, bits: (0, 0, j))
    return pl.pallas_call(
        functools.partial(weight_kernel, pieces, blocks, width, turn),
        out_shape=(out, out),
        grid_spec=pltpu.PrefetchScalarGridSpec(
            num_scalar_prefetch=1,
            grid=(pl.cdiv(columns, tile),),
            in_specs=[pl.BlockSpec(shape, where) for _, shape, where in lefts]
            + [
                pl.BlockSpec((tile, cells) if turn else (cells, tile), where)
                for _, cells, where in rights
            ],
            out_specs=[out_spec, out_spec],
            scratch_shapes=[pltpu.VMEM((rows, depth), jnp.bfloat16)],
        ),
        compiler_params=pltpu.CompilerParams(vmem_limit_bytes=20 * 1024 * 1024),
        cost_estimate=pl.CostEstimate(
            flops=2 * rows * depth * columns,
            bytes_accessed=2 * (rows * depth + depth * columns + rows * columns),
            transcendentals=0,
        ),
    )(bits, *[left[0] for left in lefts], *[right[0] for right in rights])


def summed(terms):
    total = terms[0].astype(jnp.float32)
    for term in terms[1:]:
        total = total + term.astype(jnp.float32)
    return total


def along(terms, bit, place):
    return [lax.dynamic_index_in_dim(term, bit, place, keepdims=False) for term in terms]


def stride_bit(stride):
    return (lax.axis_index("dp") >> (stride.bit_length() - 1)) & 1


def exchange(groups, stride, place):
    bit = stride_bit(stride)
    going = [summed(along(terms, 1 - bit, place)).astype(jnp.bfloat16) for terms in groups]
    joined = jnp.concatenate(going, axis=-1) if len(going) > 1 else going[0]
    shape = joined.shape
    came = swap(joined.reshape((-1,) + shape[-2:]), "dp", stride).reshape(shape)
    result, start = [], 0
    for terms, part in zip(groups, going):
        width = part.shape[-1]
        piece = lax.slice_in_dim(came, start, start + width, axis=came.ndim - 1)
        result.append(along(terms, bit, place) + [piece])
        start += width
    return result


def crossed(groups, near, far, ahead):
    size = lax.axis_size("dp")
    index = lax.axis_index("dp")
    even = index & 1 == 0
    low, high = stride_bit(near), stride_bit(far)
    own, other = jnp.where(even, low, high), jnp.where(even, high, low)

    def hop(values, first):
        strides = (near, far) if first else (far, near)
        pairs = [(i, i ^ strides[i % 2]) for i in range(size)]
        flat = values.reshape((-1,) + values.shape[-2:])
        return lax.ppermute(flat, "dp", pairs).reshape(values.shape)

    def picked(terms, mine, rest):
        place = terms[0].ndim - 3
        return along(
            along(terms, jnp.where(even, mine, rest), place),
            jnp.where(even, rest, mine),
            place - 1,
        )

    def joined(mine, rest):
        sums = [summed(picked(terms, mine, rest)) for terms in groups]
        return jnp.concatenate(sums, axis=-1) if len(sums) > 1 else sums[0]

    if ahead:
        onward = joined(1 - own, 1 - other).astype(jnp.bfloat16)
        onward = hop(onward, True)
        stays = joined(1 - own, other).astype(jnp.bfloat16)
        stays = hop(stays, True)
    else:
        both = jnp.stack([joined(1 - own, 1 - other), joined(1 - own, other)])
        both = both.astype(jnp.bfloat16)
        both = hop(both, True)
        onward, stays = both[0], both[1]
    going = (joined(own, 1 - other) + onward.astype(jnp.float32)).astype(jnp.bfloat16)
    last = hop(going, False)
    result, start = [], 0
    for terms in groups:
        width = terms[0].shape[-1]
        came = [lax.slice_in_dim(t, start, start + width, axis=t.ndim - 1) for t in (stays, last)]
        result.append(picked(terms, own, other) + came)
        start += width
    return result


def open_terms(kept, sent):
    received = swap(sent, "dp", 1)
    bits = kept.shape[0].bit_length() - 1
    shape = (2,) * bits + kept.shape[1:]
    return [kept.reshape(shape), received.reshape(shape)]


def reduce_rows(groups, strides, ahead=False):
    for stride in strides:
        if stride == 4 and 8 in strides:
            groups = crossed(groups, 4, 8, ahead)
        elif stride != 8 or 4 not in strides:
            place = groups[0][0].ndim - 3
            groups = exchange(groups, stride, place)
    return [summed(terms) for terms in groups]


def sum_all(values):
    for axis in ("gene", "dp"):
        stride = 1
        while stride < lax.axis_size(axis):
            values = values + swap(values, axis, stride)
            stride *= 2
    return values


def layer(
    counts,
    coords,
    segments,
    noise,
    embed_table,
    ln1_gain,
    ln1_bias,
    w_qkv,
    w_out,
    ln2_gain,
    ln2_bias,
    w_up,
    w_down,
    w_latent,
    mix_means,
    mix_logits,
    w_decode,
):
    cells = coords.shape[0]
    all_cells = cells * lax.axis_size("dp") * lax.axis_size("gene")
    factor = 1.0 / (all_cells * G)
    scale = HDIM ** (-0.5)
    groups = lax.axis_size("dp")
    index = lax.axis_index("dp")
    gene = lax.axis_index("gene")
    core = index & 1
    side = (index >> 1) & 1
    bits = jnp.stack([core, gene]).astype(jnp.int32)
    strides = [2**i for i in range(1, groups.bit_length() - 1)]
    expr_low, partial = embed_cells(counts.T, embed_table, 1152)
    embedded = half(partial, gene, 0) + swap(
        half(partial, 1 - gene, 0).astype(jnp.bfloat16), "gene", 1
    ).astype(jnp.float32)
    expr_side = swap(expr_low, "dp", 2)
    state_in = embedded + position_code(coords)
    normed1, unit1, spread1 = norm_forward(state_in, ln1_gain, ln1_bias)
    normed1 = normed1.astype(jnp.bfloat16)
    normed1_other = swap(normed1, "gene", 1)
    qkv_low = contract(normed1, w_qkv, ((1,), (0,))).astype(jnp.bfloat16)
    query = qkv_low[:, :D].reshape(cells, HEADS, HDIM)
    keys = qkv_low[:, D : 2 * D].reshape(cells, HEADS, HDIM)
    values = qkv_low[:, 2 * D :].reshape(cells, HEADS, HDIM)
    slide = segments[0]
    same = (slide[:, None] == slide[None, :])[None]
    scores = jnp.einsum("qhd,khd->hqk", query, keys, preferred_element_type=jnp.float32) * scale
    scores = jnp.where(same, scores, mask_floor)
    peak = jnp.max(scores, axis=-1, keepdims=True)
    expo = jnp.exp(scores - peak)
    probs = expo / jnp.sum(expo, axis=-1, keepdims=True)
    probs_low = probs.astype(jnp.bfloat16)
    attended = jnp.einsum("hqk,khd->qhd", probs_low, values, preferred_element_type=jnp.float32)
    attended = attended.reshape(cells, D).astype(jnp.bfloat16)
    state_mid = state_in + product(attended, w_out)
    attended_other = swap(attended, "gene", 1)
    normed2, unit2, spread2 = norm_forward(state_mid, ln2_gain, ln2_bias)
    normed2 = normed2.astype(jnp.bfloat16)
    normed2_other = swap(normed2, "gene", 1)
    pre_act = contract(normed2, w_up, ((1,), (0,)))
    cumul = 0.5 * (1.0 + lax.erf(pre_act * root_half))
    active = (pre_act * cumul).astype(jnp.bfloat16)
    state_out = state_mid + contract(active, w_down, ((1,), (0,)))
    out_low = state_out.astype(jnp.bfloat16)
    latent = contract(out_low, w_latent, ((1,), (0,)))
    center = latent[:, :LAT]
    log_var = latent[:, LAT:]
    deviation = jnp.exp(0.5 * log_var)
    sample = center + deviation * noise
    sample_low = sample.astype(jnp.bfloat16)
    sample_other = swap(sample_low, "gene", 1)
    active_other = swap(active, "gene", 1)
    sample_all = jnp.concatenate(
        [
            jnp.where(gene == 0, sample_low, sample_other),
            jnp.where(gene == 0, sample_other, sample_low),
        ],
        axis=0,
    )
    genes = expr_low.shape[0]
    whole = lambda j, bits: (0, 0)
    tiles = lambda j, bits: (0, j)
    decode_send, decode_keep, partial_sample, squares = decode_genes(
        counts.T, w_decode.T, sample_all, bits, factor, groups // 2, 1152
    )
    grad_sample = half(partial_sample, gene, 0) + swap(
        half(partial_sample, 1 - gene, 0).astype(jnp.bfloat16), "gene", 1
    ).astype(jnp.float32)
    decode_terms = open_terms(decode_keep, decode_send)
    (decode_part,) = reduce_rows([decode_terms], strides)
    log_weight = jax.nn.log_softmax(mix_logits)
    dist = (
        jnp.sum(sample * sample, axis=1, keepdims=True)
        - 2.0 * precise(sample, mix_means.T)
        + jnp.sum(mix_means * mix_means, axis=1)[None, :]
    )
    mix_score = log_weight[None, :] - 0.5 * dist
    top = jnp.max(mix_score, axis=1, keepdims=True)
    shifted = jnp.exp(mix_score - top)
    totals = jnp.sum(shifted, axis=1, keepdims=True)
    share = shifted / totals
    mixture = jnp.sum(-0.5 * log_var) - jnp.sum(top + jnp.log(totals))
    recon = 0.5 * jnp.sum(squares)
    loss_part = factor * (recon + mixture)
    grad_sample = grad_sample + factor * (sample - precise(share, mix_means))
    share_sum = jnp.sum(share, axis=0)
    grad_means_local = factor * (share_sum[:, None] * mix_means - precise(share.T, sample))
    weight_sum = -factor * share_sum
    grad_logits_local = weight_sum - jnp.exp(log_weight) * jnp.sum(weight_sum)
    grad_logvar = -0.5 * factor + grad_sample * 0.5 * deviation * noise
    grad_lat_low = jnp.concatenate([grad_sample, grad_logvar], axis=1).astype(jnp.bfloat16)
    out_low_other = swap(out_low, "gene", 1)

    def block_grad(left, left_other, right, tile, halved):
        columns = right.shape[1] // 2
        steps = columns // tile
        mine = lambda j, bits: (0, bits[1] * steps + j)
        going = half(lax.optimization_barrier(right), 1 - gene, 1) if halved else right
        other = swap(going, "gene", 1)
        sent, kept = weight_grad(
            [(left, left.shape, whole), (left_other, left.shape, whole)],
            [(right, cells, mine), (other, cells, tiles if halved else mine)],
            bits,
            groups // 2,
            tile,
            columns,
        )
        return open_terms(kept, sent)

    terms_latent = block_grad(out_low, out_low_other, grad_lat_low, 512, False)
    grad_state = contract(grad_lat_low, w_latent, ((1,), (1,)))
    grad_branch = grad_state.astype(jnp.bfloat16)
    terms_down = block_grad(active, active_other, grad_branch, 256, False)
    grad_active = contract(grad_branch, w_down, ((1,), (1,)))
    slope = cumul + pre_act * jnp.exp(-0.5 * pre_act * pre_act) * inv_root_two_pi
    grad_pre = (grad_active * slope).astype(jnp.bfloat16)
    terms_up = block_grad(normed2, normed2_other, grad_pre, 512, True)
    grad_normed2 = contract(grad_pre, w_up, ((1,), (1,)))
    back_two, grad_gain2, grad_bias2 = norm_backward(grad_normed2, unit2, spread2, ln2_gain)
    grad_state = grad_state + back_two
    grad_attn_low = grad_state.astype(jnp.bfloat16)
    terms_out = block_grad(attended, attended_other, grad_attn_low, 512, False)
    grad_attended = (
        contract(grad_attn_low, w_out, ((1,), (1,))).astype(jnp.bfloat16).reshape(cells, HEADS, HDIM)
    )
    grad_probs = jnp.einsum(
        "qhd,khd->hqk", grad_attended, values, preferred_element_type=jnp.float32
    )
    row_inner = jnp.sum(probs * grad_probs, axis=-1, keepdims=True)
    grad_scores = (probs * (grad_probs - row_inner)).astype(jnp.bfloat16)
    grad_query = (
        jnp.einsum("hqk,khd->qhd", grad_scores, keys, preferred_element_type=jnp.float32) * scale
    )
    grad_keys = (
        jnp.einsum("hqk,qhd->khd", grad_scores, query, preferred_element_type=jnp.float32)
        * scale
    )
    grad_values = jnp.einsum(
        "hqk,qhd->khd", probs_low, grad_attended, preferred_element_type=jnp.float32
    )
    grad_qkv_low = jnp.concatenate(
        [grad_query.reshape(cells, D), grad_keys.reshape(cells, D), grad_values.reshape(cells, D)],
        axis=1,
    ).astype(jnp.bfloat16)
    terms_qkv = block_grad(normed1, normed1_other, grad_qkv_low, 512, True)
    grad_normed1 = contract(grad_qkv_low, w_qkv, ((1,), (1,)))
    back_one, grad_gain1, grad_bias1 = norm_backward(grad_normed1, unit1, spread1, ln1_gain)
    grad_input = grad_state + back_one
    grad_embed_low = grad_input.astype(jnp.bfloat16)
    embed_mine = column_blocks(grad_embed_low, side, groups // 4)
    embed_side = swap(column_blocks(grad_embed_low, 1 - side, groups // 4), "dp", 2)
    embed_pair = jnp.stack([embed_mine, embed_side])
    embed_other = swap(embed_pair, "gene", 1)
    rows = embed_mine.shape[1]
    table_send, table_keep = weight_grad(
        [
            (embed_pair, (None, cells, rows), lambda j, bits: (0, 0, 0)),
            (embed_other, (None, cells, rows), lambda j, bits: (0, 0, 0)),
            (embed_pair, (None, cells, rows), lambda j, bits: (1, 0, 0)),
            (embed_other, (None, cells, rows), lambda j, bits: (1, 0, 0)),
        ],
        [
            (expr_low, cells, lambda j, bits: (j, bits[1])),
            (expr_low, cells, lambda j, bits: (j, 1 - bits[1])),
            (expr_side, cells, lambda j, bits: (j, bits[1])),
            (expr_side, cells, lambda j, bits: (j, 1 - bits[1])),
        ],
        bits,
        groups // 4,
        1152,
        genes,
        turn=True,
    )
    parts = (
        grad_means_local,
        jnp.stack([grad_gain1, grad_bias1, grad_gain2, grad_bias2]),
        loss_part,
        grad_logits_local,
    )
    parts, _ = lax.optimization_barrier((parts, table_send))
    means_part, norm_parts, loss_part, logits_part = parts
    count = logits_part.shape[0]
    (sum_down,) = reduce_rows([terms_down], strides)
    (sum_up,) = reduce_rows([terms_up], strides)
    sum_latent, sum_out, sum_qkv = reduce_rows([terms_latent, terms_out, terms_qkv], strides)
    table_terms = open_terms(table_keep, table_send)
    (table_part,) = reduce_rows([table_terms], strides[1:], ahead=True)
    small = jnp.concatenate(
        [
            loss_part.reshape(1, 1),
            logits_part.reshape(1, count),
            jnp.zeros((1, LAT - 1 - count), jnp.float32),
        ],
        axis=1,
    )
    stats = sum_all(
        jnp.concatenate([means_part, norm_parts.reshape(4 * (D // LAT), LAT), small], axis=0)
    )
    means_total = stats[:count]
    norms = stats[count:-1].reshape(4, D)
    sum_gain1, sum_bias1, sum_gain2, sum_bias2 = norms[0], norms[1], norms[2], norms[3]
    loss_total = stats[-1, 0]
    logits_total = stats[-1, 1 : 1 + count]
    return (
        state_out.astype(jnp.bfloat16),
        loss_total,
        grad_input,
        table_part,
        decode_part,
        sum_qkv,
        sum_out,
        sum_gain1,
        sum_bias1,
        sum_gain2,
        sum_bias2,
        sum_up,
        sum_down,
        sum_latent,
        means_total,
        logits_total,
    )


def solution(mesh):
    in_specs = (
        P("dp", "gene"),
        P(("dp", "gene"), None),
        P(("dp", "gene"), None),
        P(("dp", "gene"), None),
        P("gene", None),
        P(),
        P(),
        P(),
        P(),
        P(),
        P(),
        P(),
        P(),
        P(),
        P(),
        P(),
        P(None, "gene"),
    )
    out_specs = (
        P(("dp", "gene"), None),
        P(),
        P(("dp", "gene"), None),
        P("dp", "gene"),
        P("dp", "gene"),
        P("dp", "gene"),
        P("dp", "gene"),
        P(),
        P(),
        P(),
        P(),
        P("dp", "gene"),
        P("dp", "gene"),
        P("dp", "gene"),
        P(),
        P(),
    )
    return jax.shard_map(layer, mesh=mesh, in_specs=in_specs, out_specs=out_specs, check_vma=False)
```

```python
import functools
import math

import jax
import jax.numpy as jnp
from jax import lax
from jax.experimental import pallas as pl
from jax.experimental.pallas import tpu as pltpu
from jax.sharding import PartitionSpec as P


D = 1024
HEADS = 16
HDIM = 64
LAT = 512
G = 13500


ln_eps = 1e-05
root_half = 0.7071067811865476
inv_root_two_pi = 0.3989422804014327
mask_floor = -1e30


def product(left, right):
    return jnp.dot(left, right, preferred_element_type=jnp.float32)


def precise(left, right):
    return jnp.dot(left, right, precision=lax.Precision.HIGHEST, preferred_element_type=jnp.float32)


def position_code(coords):
    quarter = D // 4
    freq = jnp.exp(-jnp.arange(quarter, dtype=jnp.float32) * (math.log(100.0) / quarter))
    along_x = coords[:, 0:1] * freq[None, :]
    along_y = coords[:, 1:2] * freq[None, :]
    return jnp.concatenate(
        [jnp.sin(along_x), jnp.cos(along_x), jnp.sin(along_y), jnp.cos(along_y)], axis=1
    )


def norm_forward(values, gain, bias):
    center = values - jnp.mean(values, axis=-1, keepdims=True)
    spread = lax.rsqrt(jnp.mean(center * center, axis=-1, keepdims=True) + ln_eps)
    normal = center * spread
    return (normal * gain + bias, normal, spread)


def norm_backward(grad_out, normal, spread, gain):
    grad_normal = grad_out * gain
    inner = (
        grad_normal
        - jnp.mean(grad_normal, axis=-1, keepdims=True)
        - normal * jnp.mean(grad_normal * normal, axis=-1, keepdims=True)
    )
    return (spread * inner, jnp.sum(grad_out * normal, axis=0), jnp.sum(grad_out, axis=0))


def swap(values, axis, stride):
    size = lax.axis_size(axis)
    return lax.ppermute(values, axis, [(i, i ^ stride) for i in range(size)])


def contract(left, right, dims):
    return lax.dot_general(
        left, right, ((dims[0], dims[1]), ((), ())), preferred_element_type=jnp.float32
    )


def half(values, bit, axis):
    size = values.shape[axis] // 2
    low = lax.slice_in_dim(values, 0, size, axis=axis)
    high = lax.slice_in_dim(values, size, 2 * size, axis=axis)
    return jnp.where(bit == 0, low, high)


def column_blocks(values, bit, parts):
    width = values.shape[1] // (2 * parts)
    chosen = []
    for i in range(parts):
        low = values[:, 2 * i * width : (2 * i + 1) * width]
        high = values[:, (2 * i + 1) * width : (2 * i + 2) * width]
        chosen.append(jnp.where(bit == 0, low, high))
    return jnp.concatenate(chosen, axis=1)


def weight_kernel(pieces, blocks, width, turn, bits, *refs):
    lefts, rights = refs[:pieces], refs[pieces : 2 * pieces]
    send, keep, turned = refs[2 * pieces :]

    @pl.when(pl.program_id(0) == 0)
    def _():
        turned[...] = jnp.concatenate([ref[...] for ref in lefts], axis=0).T

    right = jnp.concatenate([ref[...] for ref in rights], axis=1 if turn else 0)
    total = lax.dot_general(
        turned[...],
        right,
        (((1,), (1 if turn else 0,)), ((), ())),
        preferred_element_type=jnp.float32,
    )
    first = bits[0] == 0
    for i in range(blocks):
        low = total[2 * i * width : (2 * i + 1) * width]
        high = total[(2 * i + 1) * width : (2 * i + 2) * width]
        keep[i] = jnp.where(first, low, high).astype(jnp.bfloat16)
        send[i] = jnp.where(first, high, low).astype(jnp.bfloat16)


def in_place(values):
    return pltpu.with_memory_space_constraint(values, pltpu.HBM)


def inside(tile, genes):
    row = lax.broadcasted_iota(jnp.int32, (tile, 1), 0) + pl.program_id(0) * tile
    return row < genes


def embed_kernel(genes, counts, table, expr, total):
    tile = counts.shape[0]
    valid = inside(tile, genes)
    logs = jnp.where(valid, jnp.log(1.0 + counts[...].astype(jnp.float32)), 0.0)
    low = logs.astype(jnp.bfloat16)
    expr[...] = low
    rows = jnp.where(valid, table[...], jnp.zeros_like(table[...]))
    part = jnp.dot(low.T, rows, preferred_element_type=jnp.float32)

    @pl.when(pl.program_id(0) == 0)
    def _():
        total[...] = part

    @pl.when(pl.program_id(0) > 0)
    def _():
        total[...] += part


def embed_cells(counts, table, tile):
    genes, cells = counts.shape
    width = table.shape[1]
    return pl.pallas_call(
        functools.partial(embed_kernel, genes),
        out_shape=(
            jax.ShapeDtypeStruct((genes, cells), jnp.bfloat16),
            jax.ShapeDtypeStruct((cells, width), jnp.float32),
        ),
        grid=(pl.cdiv(genes, tile),),
        in_specs=[
            pl.BlockSpec((tile, cells), lambda j: (j, 0)),
            pl.BlockSpec((tile, width), lambda j: (j, 0)),
        ],
        out_specs=[
            pl.BlockSpec((tile, cells), lambda j: (j, 0)),
            pl.BlockSpec((cells, width), lambda j: (0, 0)),
        ],
        compiler_params=pltpu.CompilerParams(vmem_limit_bytes=24 * 1024 * 1024),
        cost_estimate=pl.CostEstimate(
            flops=2 * genes * cells * width,
            bytes_accessed=genes * (6 * cells + 2 * width),
            transcendentals=genes * cells,
        ),
        name="e",
    )(in_place(counts), in_place(table))


def decode_kernel(genes, factor, blocks, width, bits, counts, table, sample, *refs):
    send, keep, grad, square, turned = refs
    tile = counts.shape[0]
    start = pl.program_id(0) == 0

    @pl.when(start)
    def _():
        turned[...] = sample[...].T
        grad[...] = jnp.zeros_like(grad)
        square[...] = jnp.zeros_like(square)

    valid = inside(tile, genes)
    rows = jnp.where(valid, table[...], jnp.zeros_like(table[...]))
    predicted = jnp.dot(rows, turned[...], preferred_element_type=jnp.float32)
    logs = jnp.log(1.0 + counts[...].astype(jnp.float32))
    error = jnp.where(valid, predicted - logs, 0.0)
    square[...] += jnp.sum(error * error, axis=0, keepdims=True)
    low = (factor * error).astype(jnp.bfloat16).T
    grad[...] += jnp.dot(low, rows, preferred_element_type=jnp.float32)
    total = jnp.dot(turned[...], low, preferred_element_type=jnp.float32)
    first = bits[0] == 0
    for i in range(blocks):
        even = total[2 * i * width : (2 * i + 1) * width]
        odd = total[(2 * i + 1) * width : (2 * i + 2) * width]
        keep[i] = jnp.where(first, even, odd).astype(jnp.bfloat16)
        send[i] = jnp.where(first, odd, even).astype(jnp.bfloat16)


def decode_genes(counts, table, sample, bits, factor, blocks, tile):
    genes, cells = counts.shape
    latents = sample.shape[1]
    width = latents // (2 * blocks)
    halves = jax.ShapeDtypeStruct((blocks, width, genes), jnp.bfloat16)
    half_spec = pl.BlockSpec((blocks, width, tile), lambda j, bits: (0, 0, j))
    whole = lambda j, bits: (0, 0)
    rows = lambda j, bits: (j, 0)
    return pl.pallas_call(
        functools.partial(decode_kernel, genes, factor, blocks, width),
        out_shape=(
            halves,
            halves,
            jax.ShapeDtypeStruct((cells, latents), jnp.float32),
            jax.ShapeDtypeStruct((1, cells), jnp.float32),
        ),
        grid_spec=pltpu.PrefetchScalarGridSpec(
            num_scalar_prefetch=1,
            grid=(pl.cdiv(genes, tile),),
            in_specs=[
                pl.BlockSpec((tile, cells), rows),
                pl.BlockSpec((tile, latents), rows),
                pl.BlockSpec((cells, latents), whole),
            ],
            out_specs=[
                half_spec,
                half_spec,
                pl.BlockSpec((cells, latents), whole),
                pl.BlockSpec((1, cells), whole),
            ],
            scratch_shapes=[pltpu.VMEM((latents, cells), jnp.bfloat16)],
        ),
        compiler_params=pltpu.CompilerParams(vmem_limit_bytes=24 * 1024 * 1024),
        cost_estimate=pl.CostEstimate(
            flops=6 * genes * cells * latents,
            bytes_accessed=genes * (4 * cells + 4 * latents),
            transcendentals=genes * cells,
        ),
        name="d",
    )(bits, in_place(counts), in_place(table), sample)


def weight_grad(lefts, rights, bits, blocks, tile, columns, turn=False):
    pieces = len(lefts)
    rows = lefts[0][1][-1]
    depth = sum(left[1][-2] for left in lefts)
    width = rows // (2 * blocks)
    out = jax.ShapeDtypeStruct((blocks, width, columns), jnp.bfloat16)
    out_spec = pl.BlockSpec((blocks, width, tile), lambda j, bits: (0, 0, j))
    return pl.pallas_call(
        functools.partial(weight_kernel, pieces, blocks, width, turn),
        out_shape=(out, out),
        grid_spec=pltpu.PrefetchScalarGridSpec(
            num_scalar_prefetch=1,
            grid=(pl.cdiv(columns, tile),),
            in_specs=[pl.BlockSpec(shape, where) for _, shape, where in lefts]
            + [
                pl.BlockSpec((tile, cells) if turn else (cells, tile), where)
                for _, cells, where in rights
            ],
            out_specs=[out_spec, out_spec],
            scratch_shapes=[pltpu.VMEM((rows, depth), jnp.bfloat16)],
        ),
        compiler_params=pltpu.CompilerParams(vmem_limit_bytes=20 * 1024 * 1024),
        cost_estimate=pl.CostEstimate(
            flops=2 * rows * depth * columns,
            bytes_accessed=2 * (rows * depth + depth * columns + rows * columns),
            transcendentals=0,
        ),
    )(bits, *[left[0] for left in lefts], *[right[0] for right in rights])


def summed(terms):
    total = terms[0].astype(jnp.float32)
    for term in terms[1:]:
        total = total + term.astype(jnp.float32)
    return total


def along(terms, bit, place):
    return [lax.dynamic_index_in_dim(term, bit, place, keepdims=False) for term in terms]


def stride_bit(stride):
    return (lax.axis_index("dp") >> (stride.bit_length() - 1)) & 1


def exchange(groups, stride, place):
    bit = stride_bit(stride)
    going = [summed(along(terms, 1 - bit, place)).astype(jnp.bfloat16) for terms in groups]
    joined = jnp.concatenate(going, axis=-1) if len(going) > 1 else going[0]
    shape = joined.shape
    came = swap(joined.reshape((-1,) + shape[-2:]), "dp", stride).reshape(shape)
    result, start = [], 0
    for terms, part in zip(groups, going):
        width = part.shape[-1]
        piece = lax.slice_in_dim(came, start, start + width, axis=came.ndim - 1)
        result.append(along(terms, bit, place) + [piece])
        start += width
    return result


def crossed(groups, near, far, ahead):
    size = lax.axis_size("dp")
    index = lax.axis_index("dp")
    even = index & 1 == 0
    low, high = stride_bit(near), stride_bit(far)
    own, other = jnp.where(even, low, high), jnp.where(even, high, low)

    def hop(values, first):
        strides = (near, far) if first else (far, near)
        pairs = [(i, i ^ strides[i % 2]) for i in range(size)]
        flat = values.reshape((-1,) + values.shape[-2:])
        return lax.ppermute(flat, "dp", pairs).reshape(values.shape)

    def picked(terms, mine, rest):
        place = terms[0].ndim - 3
        return along(
            along(terms, jnp.where(even, mine, rest), place),
            jnp.where(even, rest, mine),
            place - 1,
        )

    def joined(mine, rest):
        sums = [summed(picked(terms, mine, rest)) for terms in groups]
        return jnp.concatenate(sums, axis=-1) if len(sums) > 1 else sums[0]

    if ahead:
        onward = joined(1 - own, 1 - other).astype(jnp.bfloat16)
        onward = hop(onward, True)
        stays = joined(1 - own, other).astype(jnp.bfloat16)
        stays = hop(stays, True)
    else:
        both = jnp.stack([joined(1 - own, 1 - other), joined(1 - own, other)])
        both = both.astype(jnp.bfloat16)
        both = hop(both, True)
        onward, stays = both[0], both[1]
    going = (joined(own, 1 - other) + onward.astype(jnp.float32)).astype(jnp.bfloat16)
    last = hop(going, False)
    result, start = [], 0
    for terms in groups:
        width = terms[0].shape[-1]
        came = [lax.slice_in_dim(t, start, start + width, axis=t.ndim - 1) for t in (stays, last)]
        result.append(picked(terms, own, other) + came)
        start += width
    return result


def open_terms(kept, sent):
    received = swap(sent, "dp", 1)
    bits = kept.shape[0].bit_length() - 1
    shape = (2,) * bits + kept.shape[1:]
    return [kept.reshape(shape), received.reshape(shape)]


def reduce_rows(groups, strides, ahead=False):
    for stride in strides:
        if stride == 4 and 8 in strides:
            groups = crossed(groups, 4, 8, ahead)
        elif stride != 8 or 4 not in strides:
            place = groups[0][0].ndim - 3
            groups = exchange(groups, stride, place)
    return [summed(terms) for terms in groups]


def sum_all(values):
    for axis in ("gene", "dp"):
        stride = 1
        while stride < lax.axis_size(axis):
            values = values + swap(values, axis, stride)
            stride *= 2
    return values


def layer(
    counts,
    coords,
    segments,
    noise,
    embed_table,
    ln1_gain,
    ln1_bias,
    w_qkv,
    w_out,
    ln2_gain,
    ln2_bias,
    w_up,
    w_down,
    w_latent,
    mix_means,
    mix_logits,
    w_decode,
):
    cells = coords.shape[0]
    all_cells = cells * lax.axis_size("dp") * lax.axis_size("gene")
    factor = 1.0 / (all_cells * G)
    scale = HDIM ** (-0.5)
    groups = lax.axis_size("dp")
    index = lax.axis_index("dp")
    gene = lax.axis_index("gene")
    core = index & 1
    side = (index >> 1) & 1
    bits = jnp.stack([core, gene]).astype(jnp.int32)
    strides = [2**i for i in range(1, groups.bit_length() - 1)]
    expr_low, partial = embed_cells(counts.T, embed_table, 768)
    embedded = half(partial, gene, 0) + swap(
        half(partial, 1 - gene, 0).astype(jnp.bfloat16), "gene", 1
    ).astype(jnp.float32)
    expr_side = swap(expr_low, "dp", 2)
    state_in = embedded + position_code(coords)
    normed1, unit1, spread1 = norm_forward(state_in, ln1_gain, ln1_bias)
    normed1 = normed1.astype(jnp.bfloat16)
    normed1_other = swap(normed1, "gene", 1)
    qkv_low = contract(normed1, w_qkv, ((1,), (0,))).astype(jnp.bfloat16)
    query = qkv_low[:, :D].reshape(cells, HEADS, HDIM)
    keys = qkv_low[:, D : 2 * D].reshape(cells, HEADS, HDIM)
    values = qkv_low[:, 2 * D :].reshape(cells, HEADS, HDIM)
    slide = segments[0]
    same = (slide[:, None] == slide[None, :])[None]
    scores = jnp.einsum("qhd,khd->hqk", query, keys, preferred_element_type=jnp.float32) * scale
    scores = jnp.where(same, scores, mask_floor)
    peak = jnp.max(scores, axis=-1, keepdims=True)
    expo = jnp.exp(scores - peak)
    probs = expo / jnp.sum(expo, axis=-1, keepdims=True)
    probs_low = probs.astype(jnp.bfloat16)
    attended = jnp.einsum("hqk,khd->qhd", probs_low, values, preferred_element_type=jnp.float32)
    attended = attended.reshape(cells, D).astype(jnp.bfloat16)
    state_mid = state_in + product(attended, w_out)
    attended_other = swap(attended, "gene", 1)
    normed2, unit2, spread2 = norm_forward(state_mid, ln2_gain, ln2_bias)
    normed2 = normed2.astype(jnp.bfloat16)
    normed2_other = swap(normed2, "gene", 1)
    pre_act = contract(normed2, w_up, ((1,), (0,)))
    cumul = 0.5 * (1.0 + lax.erf(pre_act * root_half))
    active = (pre_act * cumul).astype(jnp.bfloat16)
    state_out = state_mid + contract(active, w_down, ((1,), (0,)))
    out_low = state_out.astype(jnp.bfloat16)
    latent = contract(out_low, w_latent, ((1,), (0,)))
    center = latent[:, :LAT]
    log_var = latent[:, LAT:]
    deviation = jnp.exp(0.5 * log_var)
    sample = center + deviation * noise
    sample_low = sample.astype(jnp.bfloat16)
    sample_other = swap(sample_low, "gene", 1)
    active_other = swap(active, "gene", 1)
    sample_all = jnp.concatenate(
        [
            jnp.where(gene == 0, sample_low, sample_other),
            jnp.where(gene == 0, sample_other, sample_low),
        ],
        axis=0,
    )
    genes = expr_low.shape[0]
    whole = lambda j, bits: (0, 0)
    tiles = lambda j, bits: (0, j)
    decode_send, decode_keep, partial_sample, squares = decode_genes(
        counts.T, w_decode.T, sample_all, bits, factor, groups // 2, 768
    )
    grad_sample = half(partial_sample, gene, 0) + swap(
        half(partial_sample, 1 - gene, 0).astype(jnp.bfloat16), "gene", 1
    ).astype(jnp.float32)
    decode_terms = open_terms(decode_keep, decode_send)
    (decode_part,) = reduce_rows([decode_terms], strides)
    log_weight = jax.nn.log_softmax(mix_logits)
    dist = (
        jnp.sum(sample * sample, axis=1, keepdims=True)
        - 2.0 * precise(sample, mix_means.T)
        + jnp.sum(mix_means * mix_means, axis=1)[None, :]
    )
    mix_score = log_weight[None, :] - 0.5 * dist
    top = jnp.max(mix_score, axis=1, keepdims=True)
    shifted = jnp.exp(mix_score - top)
    totals = jnp.sum(shifted, axis=1, keepdims=True)
    share = shifted / totals
    mixture = jnp.sum(-0.5 * log_var) - jnp.sum(top + jnp.log(totals))
    recon = 0.5 * jnp.sum(squares)
    loss_part = factor * (recon + mixture)
    grad_sample = grad_sample + factor * (sample - precise(share, mix_means))
    share_sum = jnp.sum(share, axis=0)
    grad_means_local = factor * (share_sum[:, None] * mix_means - precise(share.T, sample))
    weight_sum = -factor * share_sum
    grad_logits_local = weight_sum - jnp.exp(log_weight) * jnp.sum(weight_sum)
    grad_logvar = -0.5 * factor + grad_sample * 0.5 * deviation * noise
    grad_lat_low = jnp.concatenate([grad_sample, grad_logvar], axis=1).astype(jnp.bfloat16)
    out_low_other = swap(out_low, "gene", 1)

    def block_grad(left, left_other, right, tile, halved):
        columns = right.shape[1] // 2
        steps = columns // tile
        mine = lambda j, bits: (0, bits[1] * steps + j)
        going = half(lax.optimization_barrier(right), 1 - gene, 1) if halved else right
        other = swap(going, "gene", 1)
        sent, kept = weight_grad(
            [(left, left.shape, whole), (left_other, left.shape, whole)],
            [(right, cells, mine), (other, cells, tiles if halved else mine)],
            bits,
            groups // 2,
            tile,
            columns,
        )
        return open_terms(kept, sent)

    terms_latent = block_grad(out_low, out_low_other, grad_lat_low, 256, False)
    grad_state = contract(grad_lat_low, w_latent, ((1,), (1,)))
    grad_branch = grad_state.astype(jnp.bfloat16)
    terms_down = block_grad(active, active_other, grad_branch, 256, False)
    grad_active = contract(grad_branch, w_down, ((1,), (1,)))
    slope = cumul + pre_act * jnp.exp(-0.5 * pre_act * pre_act) * inv_root_two_pi
    grad_pre = (grad_active * slope).astype(jnp.bfloat16)
    terms_up = block_grad(normed2, normed2_other, grad_pre, 256, True)
    grad_normed2 = contract(grad_pre, w_up, ((1,), (1,)))
    back_two, grad_gain2, grad_bias2 = norm_backward(grad_normed2, unit2, spread2, ln2_gain)
    grad_state = grad_state + back_two
    grad_attn_low = grad_state.astype(jnp.bfloat16)
    terms_out = block_grad(attended, attended_other, grad_attn_low, 256, False)
    grad_attended = (
        contract(grad_attn_low, w_out, ((1,), (1,))).astype(jnp.bfloat16).reshape(cells, HEADS, HDIM)
    )
    grad_probs = jnp.einsum(
        "qhd,khd->hqk", grad_attended, values, preferred_element_type=jnp.float32
    )
    row_inner = jnp.sum(probs * grad_probs, axis=-1, keepdims=True)
    grad_scores = (probs * (grad_probs - row_inner)).astype(jnp.bfloat16)
    grad_query = (
        jnp.einsum("hqk,khd->qhd", grad_scores, keys, preferred_element_type=jnp.float32) * scale
    )
    grad_keys = (
        jnp.einsum("hqk,qhd->khd", grad_scores, query, preferred_element_type=jnp.float32)
        * scale
    )
    grad_values = jnp.einsum(
        "hqk,qhd->khd", probs_low, grad_attended, preferred_element_type=jnp.float32
    )
    grad_qkv_low = jnp.concatenate(
        [grad_query.reshape(cells, D), grad_keys.reshape(cells, D), grad_values.reshape(cells, D)],
        axis=1,
    ).astype(jnp.bfloat16)
    terms_qkv = block_grad(normed1, normed1_other, grad_qkv_low, 256, True)
    grad_normed1 = contract(grad_qkv_low, w_qkv, ((1,), (1,)))
    back_one, grad_gain1, grad_bias1 = norm_backward(grad_normed1, unit1, spread1, ln1_gain)
    grad_input = grad_state + back_one
    grad_embed_low = grad_input.astype(jnp.bfloat16)
    embed_mine = column_blocks(grad_embed_low, side, groups // 4)
    embed_side = swap(column_blocks(grad_embed_low, 1 - side, groups // 4), "dp", 2)
    embed_pair = jnp.stack([embed_mine, embed_side])
    embed_other = swap(embed_pair, "gene", 1)
    rows = embed_mine.shape[1]
    table_send, table_keep = weight_grad(
        [
            (embed_pair, (None, cells, rows), lambda j, bits: (0, 0, 0)),
            (embed_other, (None, cells, rows), lambda j, bits: (0, 0, 0)),
            (embed_pair, (None, cells, rows), lambda j, bits: (1, 0, 0)),
            (embed_other, (None, cells, rows), lambda j, bits: (1, 0, 0)),
        ],
        [
            (expr_low, cells, lambda j, bits: (j, bits[1])),
            (expr_low, cells, lambda j, bits: (j, 1 - bits[1])),
            (expr_side, cells, lambda j, bits: (j, bits[1])),
            (expr_side, cells, lambda j, bits: (j, 1 - bits[1])),
        ],
        bits,
        groups // 4,
        768,
        genes,
        turn=True,
    )
    parts = (
        grad_means_local,
        jnp.stack([grad_gain1, grad_bias1, grad_gain2, grad_bias2]),
        loss_part,
        grad_logits_local,
    )
    parts, _ = lax.optimization_barrier((parts, table_send))
    means_part, norm_parts, loss_part, logits_part = parts
    count = logits_part.shape[0]
    (sum_down,) = reduce_rows([terms_down], strides)
    (sum_up,) = reduce_rows([terms_up], strides)
    sum_latent, sum_out, sum_qkv = reduce_rows([terms_latent, terms_out, terms_qkv], strides)
    table_terms = open_terms(table_keep, table_send)
    (table_part,) = reduce_rows([table_terms], strides[1:], ahead=True)
    small = jnp.concatenate(
        [
            loss_part.reshape(1, 1),
            logits_part.reshape(1, count),
            jnp.zeros((1, LAT - 1 - count), jnp.float32),
        ],
        axis=1,
    )
    stats = sum_all(
        jnp.concatenate([means_part, norm_parts.reshape(4 * (D // LAT), LAT), small], axis=0)
    )
    means_total = stats[:count]
    norms = stats[count:-1].reshape(4, D)
    sum_gain1, sum_bias1, sum_gain2, sum_bias2 = norms[0], norms[1], norms[2], norms[3]
    loss_total = stats[-1, 0]
    logits_total = stats[-1, 1 : 1 + count]
    return (
        state_out.astype(jnp.bfloat16),
        loss_total,
        grad_input,
        table_part,
        decode_part,
        sum_qkv,
        sum_out,
        sum_gain1,
        sum_bias1,
        sum_gain2,
        sum_bias2,
        sum_up,
        sum_down,
        sum_latent,
        means_total,
        logits_total,
    )


def solution(mesh):
    in_specs = (
        P("dp", "gene"),
        P(("dp", "gene"), None),
        P(("dp", "gene"), None),
        P(("dp", "gene"), None),
        P("gene", None),
        P(),
        P(),
        P(),
        P(),
        P(),
        P(),
        P(),
        P(),
        P(),
        P(),
        P(),
        P(None, "gene"),
    )
    out_specs = (
        P(("dp", "gene"), None),
        P(),
        P(("dp", "gene"), None),
        P("dp", "gene"),
        P("dp", "gene"),
        P("dp", "gene"),
        P("dp", "gene"),
        P(),
        P(),
        P(),
        P(),
        P("dp", "gene"),
        P("dp", "gene"),
        P("dp", "gene"),
        P(),
        P(),
    )
    return jax.shard_map(layer, mesh=mesh, in_specs=in_specs, out_specs=out_specs, check_vma=False)
```
